32 devices in a mesh: slab: 8 (over z, x), yz: 4 (over y, core).
Axes of the slice: x: 2, y: 2, z: 4, core: 2. Of those that a mesh axis runs over, the one named last changes fastest.
Arguments:
- embeddings: bfloat16 [512, 25, 128], P(('slab', 'yz')), may hold values from -6 to 6
- neighbours: int32 [16384], P(('slab', 'yz')), may hold values from 0 to 127
- valid: int32 [16384], P(('slab', 'yz')), may hold values 0 or 1
- azimuth: float32 [16384], P(('slab', 'yz')), may hold values from -3.140625 to 3.140625
- polar: float32 [16384], P(('slab', 'yz')), may hold values from 0 to 3.14159
- distance: float32 [16384], P(('slab', 'yz')), may hold values from 0.9 to 5
- send_low: int32 [256], P(('slab', 'yz')), may hold values from 0 to 15
- send_high: int32 [256], P(('slab', 'yz')), may hold values from 0 to 15
- w_zero: bfloat16 [2, 640, 640], replicated, may hold values from -0.25 to 0.25
- w_one_re: bfloat16 [2, 512, 512], replicated, may hold values from -0.25 to 0.25
- w_one_im: bfloat16 [2, 512, 512], replicated, may hold values from -0.25 to 0.25
- w_two_re: bfloat16 [2, 384, 384], replicated, may hold values from -0.3125 to 0.3125
- w_two_im: bfloat16 [2, 384, 384], replicated, may hold values from -0.3125 to 0.3125
- radial_weight: float32 [2, 8, 128], replicated, may hold values from -2 to 2
- readout: float32 [128], replicated, may hold values from -0.5 to 0.5
Outputs:
- updated: bfloat16 [512, 25, 128], P(('slab', 'yz'))
- forces: float32 [3, 512], P(None, ('slab', 'yz'))
The draws below stay inside these ranges and needn't reach their ends.
All inputs are finite; a program needn't handle non-finite values. No bound on the sum of `valid` on one device may be relied on, other than what follows from the above.
Results may differ from the reference program's by a relative error of at most 0.0043.
Values may be sent and summed in bfloat16 or wider, within the bound.
A program may use at most 64 MiB of HBM per device.

```python
import math
import jax
import jax.numpy as jnp
from jax import lax

CHANNELS = 128
COEFFS = 25
NEIGHB = 32
LAYERS = 2
ATOM_DEV = 16
GHOSTS = 8
ATOMS = 512
EDGES = 16384
GHOST_ALL = 256
N_SLAB = 8
N_YZ = 4


def with_ends(entries, stream_key, smallest, high):
    spot = [jax.random.randint(jax.random.fold_in(stream_key, axis), (), 0, length) for axis, length in enumerate(entries.shape)]
    widest = entries.shape.index(max(entries.shape))
    neighbour = spot[:widest] + [(spot[widest] + 1) % entries.shape[widest]] + spot[widest + 1:]
    return entries.at[tuple(spot)].set(smallest).at[tuple(neighbour)].set(high)


def block_scale(rng, shape, pieces, smallest, largest):
    level, own = 1.0, jax.random.fold_in(rng, 6)
    for axis_at, parts in pieces:
        heights = jnp.exp(jax.random.uniform(jax.random.fold_in(own, axis_at), (parts,), jnp.float32, smallest / len(pieces), largest / len(pieces)))
        level = level * jnp.repeat(heights, shape[axis_at] // parts).reshape([-1 if axis == axis_at else 1 for axis in range(len(shape))])
    return level


def noise(key, dims, scale, limit, cuts=(), kind=jnp.bfloat16):
    factor_of = block_scale(key, dims, cuts, -0.22, 0.18) if cuts else 1.0
    entries = jax.random.normal(key, dims, jnp.float32) * scale * factor_of
    return jnp.minimum(jnp.maximum(entries, -limit), limit).astype(kind)


def setup_inputs(seed: int = 0) -> dict:
    keys = jax.random.split(jax.random.key(seed), 16)
    return {
        "embeddings": noise(keys[0], (ATOMS, COEFFS, CHANNELS), 1.0, 6.0, ((0, 32),)),
        "neighbours": with_ends(jax.random.randint(keys[1], (EDGES,), 0, N_YZ * (ATOM_DEV + 2 * GHOSTS)), jax.random.fold_in(keys[1], 1), 0, (N_YZ * (ATOM_DEV + 2 * GHOSTS)) - 1).astype(jnp.int32),
        "valid": with_ends((jax.random.randint(keys[2], (EDGES,), 0, 8) < 7).astype(jnp.int32), jax.random.fold_in(keys[2], 1), 0, 1),
        "azimuth": jnp.clip(jax.random.uniform(keys[3], (EDGES,), jnp.float32, -3.140625, 3.140625), -3.140625, 3.140625),
        "polar": jnp.clip(3.14159 * jax.random.uniform(keys[4], (EDGES,), jnp.float32) ** block_scale(keys[4], (EDGES,), ((0, 32),), -0.2, 0.2), 0.0, 3.14159),
        "distance": jnp.clip(0.9 + 4.1 * jax.random.uniform(keys[5], (EDGES,), jnp.float32) ** block_scale(keys[5], (EDGES,), ((0, 32),), -0.2, 0.2), 0.9, 5.0),
        "send_low": with_ends(jax.random.randint(keys[6], (GHOST_ALL,), 0, ATOM_DEV), jax.random.fold_in(keys[6], 1), 0, ATOM_DEV - 1).astype(jnp.int32),
        "send_high": with_ends(jax.random.randint(keys[7], (GHOST_ALL,), 0, ATOM_DEV), jax.random.fold_in(keys[7], 1), 0, ATOM_DEV - 1).astype(jnp.int32),
        "w_zero": noise(keys[8], (LAYERS, 5 * CHANNELS, 5 * CHANNELS), (5 * CHANNELS) ** -0.5, 0.25),
        "w_one_re": noise(keys[9], (LAYERS, 4 * CHANNELS, 4 * CHANNELS), (4 * CHANNELS) ** -0.5, 0.25),
        "w_one_im": noise(keys[10], (LAYERS, 4 * CHANNELS, 4 * CHANNELS), (4 * CHANNELS) ** -0.5, 0.25),
        "w_two_re": noise(keys[11], (LAYERS, 3 * CHANNELS, 3 * CHANNELS), (3 * CHANNELS) ** -0.5, 0.3125),
        "w_two_im": noise(keys[12], (LAYERS, 3 * CHANNELS, 3 * CHANNELS), (3 * CHANNELS) ** -0.5, 0.3125),
        "radial_weight": noise(keys[13], (LAYERS, 8, CHANNELS), 8 ** -0.5, 2.0, (), jnp.float32),
        "readout": noise(keys[14], (CHANNELS,), CHANNELS ** -0.5, 0.5, (), jnp.float32),
    }


HIGHEST = lax.Precision.HIGHEST

def slot_index(degree, azimuth_order):
    return degree * degree + degree + azimuth_order

def radial_scale(distance, radial_weight):
    centers = 1.0 + 0.5 * jnp.arange(8, dtype=jnp.float32)
    basis_values = jnp.exp(-jnp.square((distance[:, None] - centers[None, :]) / 0.5))
    return jax.nn.silu(jnp.dot(basis_values, radial_weight, precision=HIGHEST))

def stacked(values, slots):
    return jnp.stack([values[:, coeff_slot] for coeff_slot in slots], axis=1)

def convolve(features, azimuth, distance, valid, w_zero, w_one_re, w_one_im, w_two_re, w_two_im, radial_weight):
    values = features.astype(jnp.float32)
    edge_count = values.shape[0]
    channel_count = values.shape[2]
    degrees = math.isqrt(values.shape[1])
    radial_rows = (radial_scale(distance, radial_weight) * valid.astype(jnp.float32)[:, None])[:, None, :]
    results = [None] * values.shape[1]
    zero_slots = [slot_index(degree, 0) for degree in range(degrees)]
    zero_in = stacked(values, zero_slots).reshape(edge_count, -1).astype(jnp.bfloat16)
    zero_out = jnp.dot(zero_in, w_zero, preferred_element_type=jnp.float32).reshape(edge_count, degrees, channel_count) * radial_rows
    for position, coeff_slot in enumerate(zero_slots):
        results[coeff_slot] = zero_out[:, position]
    for azimuth_order, real_part, imag_part in ((1, w_one_re, w_one_im), (2, w_two_re, w_two_im)):
        plus_slots = [slot_index(degree, azimuth_order) for degree in range(azimuth_order, degrees)]
        minus_slots = [slot_index(degree, -azimuth_order) for degree in range(azimuth_order, degrees)]
        plus_part = stacked(values, plus_slots)
        minus_part = stacked(values, minus_slots)
        cosine = jnp.cos(azimuth_order * azimuth)[:, None, None]
        sine = jnp.sin(azimuth_order * azimuth)[:, None, None]
        turned_plus = (cosine * plus_part + sine * minus_part).reshape(edge_count, -1).astype(jnp.bfloat16)
        turned_minus = (cosine * minus_part - sine * plus_part).reshape(edge_count, -1).astype(jnp.bfloat16)
        out_plus = (jnp.dot(turned_plus, real_part, preferred_element_type=jnp.float32) - jnp.dot(turned_minus, imag_part, preferred_element_type=jnp.float32)).reshape(edge_count, -1, channel_count) * radial_rows
        out_minus = (jnp.dot(turned_plus, imag_part, preferred_element_type=jnp.float32) + jnp.dot(turned_minus, real_part, preferred_element_type=jnp.float32)).reshape(edge_count, -1, channel_count) * radial_rows
        back_plus = cosine * out_plus - sine * out_minus
        back_minus = sine * out_plus + cosine * out_minus
        for position, coeff_slot in enumerate(plus_slots):
            results[coeff_slot] = back_plus[:, position]
        for position, coeff_slot in enumerate(minus_slots):
            results[coeff_slot] = back_minus[:, position]
    blank = jnp.zeros((edge_count, channel_count), jnp.float32)
    full = jnp.stack([blank if entry_value is None else entry_value for entry_value in results], axis=1)
    return (full, zero_out[:, 0])

def reference(embeddings, neighbours, valid, azimuth, polar, distance, send_low, send_high, w_zero, w_one_re, w_one_im, w_two_re, w_two_im, radial_weight, readout):
    slabs = N_SLAB
    devices = N_SLAB * N_YZ
    coeffs = embeddings.shape[1]
    channel_count = embeddings.shape[2]
    table_rows = N_YZ * (ATOM_DEV + 2 * GHOSTS)
    low_lists = send_low.reshape(devices, GHOSTS)
    high_lists = send_high.reshape(devices, GHOSTS)
    slab_neighbours = neighbours.reshape(slabs, -1)
    slab_azimuth = azimuth.reshape(slabs, -1)
    slab_polar = polar.reshape(slabs, -1)
    slab_distance = distance.reshape(slabs, -1)
    slab_valid = valid.reshape(slabs, -1)
    current = embeddings
    strength = None
    for layer_index in range(LAYERS):
        device_rows = current.reshape(devices, ATOM_DEV, coeffs, channel_count)
        low_rows = jax.vmap(lambda rows, picks: rows[picks])(device_rows, low_lists).reshape(slabs, N_YZ * GHOSTS, coeffs, channel_count)
        high_rows = jax.vmap(lambda rows, picks: rows[picks])(device_rows, high_lists).reshape(slabs, N_YZ * GHOSTS, coeffs, channel_count)
        own_rows = current.reshape(slabs, N_YZ * ATOM_DEV, coeffs, channel_count)
        tables = jnp.concatenate([own_rows, jnp.roll(high_rows, 1, axis=0), jnp.roll(low_rows, -1, axis=0)], axis=1)
        weights = (w_zero[layer_index], w_one_re[layer_index], w_one_im[layer_index], w_two_re[layer_index], w_two_im[layer_index], radial_weight[layer_index])

        def per_slab(items):
            table, picks, angle, length, usable = items
            message, scalar_out = convolve(table[picks], angle, length, usable, *weights)
            summed = message.reshape(-1, NEIGHB, coeffs, channel_count).sum(axis=1)
            return (summed, 0.125 * jnp.dot(scalar_out, readout, precision=HIGHEST))
        summed, strength = lax.map(per_slab, (tables, slab_neighbours, slab_azimuth, slab_distance, slab_valid))
        current = (current.astype(jnp.float32) + 0.18 * summed.reshape(-1, coeffs, channel_count)).astype(jnp.bfloat16)
    direction = jnp.stack([jnp.sin(slab_polar) * jnp.cos(slab_azimuth), jnp.sin(slab_polar) * jnp.sin(slab_azimuth), jnp.cos(slab_polar)], axis=0)
    pull = direction * strength[None]
    own_force = pull.reshape(3, -1, NEIGHB).sum(axis=-1)

    def table_pull(items):
        slab_pull, picks = items
        onehot = (picks[:, None] == jnp.arange(table_rows, dtype=jnp.int32)[None, :]).astype(jnp.float32)
        return -jnp.dot(slab_pull, onehot, precision=HIGHEST)
    table_force = lax.map(table_pull, (jnp.transpose(pull, (1, 0, 2)), slab_neighbours))
    own_rows_count = N_YZ * ATOM_DEV
    own_part = jnp.transpose(table_force[:, :, :own_rows_count], (1, 0, 2)).reshape(3, -1)
    below_part = jnp.roll(table_force[:, :, own_rows_count:own_rows_count + N_YZ * GHOSTS], -1, axis=0)
    above_part = jnp.roll(table_force[:, :, own_rows_count + N_YZ * GHOSTS:], 1, axis=0)
    below_dev = jnp.transpose(below_part.reshape(slabs, 3, N_YZ, GHOSTS), (0, 2, 1, 3)).reshape(devices, 3, GHOSTS)
    above_dev = jnp.transpose(above_part.reshape(slabs, 3, N_YZ, GHOSTS), (0, 2, 1, 3)).reshape(devices, 3, GHOSTS)
    atom_ids = jnp.arange(ATOM_DEV, dtype=jnp.int32)
    high_hot = (high_lists[:, :, None] == atom_ids[None, None, :]).astype(jnp.float32)
    low_hot = (low_lists[:, :, None] == atom_ids[None, None, :]).astype(jnp.float32)
    ghost_force = jnp.einsum('dcg,dga->dca', below_dev, high_hot, precision=HIGHEST) + jnp.einsum('dcg,dga->dca', above_dev, low_hot, precision=HIGHEST)
    forces = own_force + own_part + jnp.transpose(ghost_force, (1, 0, 2)).reshape(3, -1)
    return (current, forces)
```

```python
import functools
import math

import jax
import jax.numpy as jnp
from jax import lax
from jax.experimental import pallas as pl
from jax.experimental.pallas import tpu as pltpu
from jax.sharding import PartitionSpec as P

LAYERS = 2
MESH = pl.DeviceIdType.MESH
HIGHEST = lax.Precision.HIGHEST
F32 = jnp.float32
BF16 = jnp.bfloat16


def slot_index(degree, order):
    return degree * degree + degree + order


def slot_groups(degrees):
    groups = [[slot_index(degree, 0) for degree in range(degrees)]]
    for order in (1, 2):
        groups.append(
            [slot_index(degree, order) for degree in range(order, degrees)]
            + [slot_index(degree, -order) for degree in range(order, degrees)]
        )
    return groups


def nt_dot(left, right, precision=None):
    return lax.dot_general(
        left, right, (((1,), (1,)), ((), ())), precision=precision, preferred_element_type=F32
    )


def kernel(
    n_slab,
    n_yz,
    atoms,
    coeffs,
    stride,
    channels,
    ghosts,
    neighb,
    groups,
    emb,
    nbr,
    val,
    azi,
    pol,
    dist,
    send_low,
    send_high,
    w_hbm0,
    w_hbm1,
    w_hbm2,
    w_hbm3,
    w_hbm4,
    radial_weight,
    readout,
    out_e,
    out_f,
    wv0,
    wv1,
    wv2,
    wv3,
    wv4,
    unpacked,
    natural,
    radp,
    picks,
    scatter,
    direction,
    f_send,
    f_recv,
    *rest,
):
    n_groups = len(groups)
    own_bufs = [rest[layer * n_groups : (layer + 1) * n_groups] for layer in range(LAYERS)]
    rest = rest[LAYERS * n_groups :]
    ghost_bufs = [rest[layer * n_groups : (layer + 1) * n_groups] for layer in range(LAYERS)]
    rest = rest[LAYERS * n_groups :]
    lend_bufs = [rest[layer * n_groups : (layer + 1) * n_groups] for layer in range(LAYERS)]
    rest = rest[LAYERS * n_groups :]
    weight_sem, send_sem, recv_sem = rest

    edges = atoms * neighb
    own_rows = n_yz * atoms
    ghost_rows = n_yz * ghosts
    table_rows = own_rows + 2 * ghost_rows
    half = n_yz // 2

    slab = lax.axis_index("slab")
    q = lax.axis_index("yz")
    above = lax.rem(slab + 1, n_slab)
    below = lax.rem(slab + n_slab - 1, n_slab)
    core = lax.rem(q, 2)
    row = q // 2
    partner = q + 1 - 2 * core

    def to_peer(j):
        return lax.rem(row + j, half) * 2 + core

    def from_peer(j):
        return lax.rem(row + half - j, half) * 2 + core

    def partner_of(index):
        return index + 1 - 2 * lax.rem(index, 2)

    weight_pairs = ((w_hbm0, wv0), (w_hbm1, wv1), (w_hbm2, wv2), (w_hbm3, wv3), (w_hbm4, wv4))
    weight_copies = [
        [
            pltpu.make_async_copy(
                source.at[layer], target.at[layer], weight_sem.at[layer * 5 + number]
            )
            for number, (source, target) in enumerate(weight_pairs)
        ]
        for layer in range(LAYERS)
    ]
    for layer in range(LAYERS):
        for copy in weight_copies[layer]:
            copy.start()

    barrier = pltpu.get_barrier_semaphore()
    peers = [(slab, lax.rem(q + j, n_yz)) for j in range(1, n_yz)]
    peers += [(above, lax.rem(q + j, n_yz)) for j in range(n_yz)]
    peers += [(below, lax.rem(q + j, n_yz)) for j in range(n_yz)]
    for peer in peers:
        pl.semaphore_signal(barrier, inc=1, device_id=peer, device_id_type=MESH)

    lend_row = lax.broadcasted_iota(jnp.int32, (2 * ghosts, atoms), 0)
    lend_col = lax.broadcasted_iota(jnp.int32, (2 * ghosts, atoms), 1)
    wanted = jnp.zeros((2 * ghosts, atoms), jnp.int32)
    for g in range(ghosts):
        wanted = jnp.where(lend_row == g, send_high[g], wanted)
        wanted = jnp.where(lend_row == ghosts + g, send_low[g], wanted)
    lend = (wanted == lend_col).astype(F32).astype(BF16)

    def lend_rows(layer, number):
        rows = jnp.dot(lend, own_bufs[layer][number][q], preferred_element_type=F32)
        lend_bufs[layer][number][0] = rows[:ghosts].astype(BF16)
        lend_bufs[layer][number][1] = rows[ghosts:].astype(BF16)

    for atom in range(atoms):
        unpacked[stride * atom : stride * atom + coeffs, :] = emb[atom].astype(F32)
    for number, group in enumerate(groups):
        for place, slot in enumerate(group):
            own_bufs[0][number][q, :, place * channels : (place + 1) * channels] = unpacked[
                pl.ds(slot, atoms, stride=stride), :
            ].astype(BF16)
        lend_rows(0, number)

    pl.semaphore_wait(barrier, len(peers))

    sends = []
    count = [0]

    def send(source, target, device):
        k = count[0]
        count[0] += 1
        copy = pltpu.make_async_remote_copy(
            src_ref=source,
            dst_ref=target,
            send_sem=send_sem.at[k],
            recv_sem=recv_sem.at[k],
            device_id=device,
            device_id_type=MESH,
        )
        copy.start()
        sends.append(copy)
        return k

    def arrive(k, target):
        pltpu.make_async_remote_copy(
            src_ref=target,
            dst_ref=target,
            send_sem=send_sem.at[k],
            recv_sem=recv_sem.at[k],
            device_id=(slab, partner),
            device_id_type=MESH,
        ).wait_recv()

    marks = {}

    def stage_a(layer, number):
        own, ghost, lent = (
            own_bufs[layer][number],
            ghost_bufs[layer][number],
            lend_bufs[layer][number],
        )
        marks["up", layer, number] = send(lent.at[0], ghost.at[q, 0], (above, q))
        marks["down", layer, number] = send(lent.at[1], ghost.at[q, 1], (below, q))
        for j in range(1, half):
            marks["own", layer, number, j] = send(own.at[q], own.at[q], (slab, to_peer(j)))
        marks["own", layer, number, 0] = send(own.at[q], own.at[q], (slab, partner))

    def stage_b(layer, number):
        own = own_bufs[layer][number]
        for j in range(1, half):
            source = from_peer(j)
            arrive(marks["own", layer, number, j], own.at[source])
            marks["own2", layer, number, j] = send(
                own.at[source], own.at[source], (slab, partner)
            )

    def stage_c(layer, number):
        ghost = ghost_bufs[layer][number]
        arrive(marks["up", layer, number], ghost.at[q, 0])
        arrive(marks["down", layer, number], ghost.at[q, 1])
        for j in range(1, half):
            marks["ghost", layer, number, j] = send(
                ghost.at[q], ghost.at[q], (slab, to_peer(j))
            )
        marks["ghost", layer, number, 0] = send(ghost.at[q], ghost.at[q], (slab, partner))

    def stage_d(layer, number):
        ghost = ghost_bufs[layer][number]
        for j in range(1, half):
            source = from_peer(j)
            arrive(marks["ghost", layer, number, j], ghost.at[source])
            marks["ghost2", layer, number, j] = send(
                ghost.at[source], ghost.at[source], (slab, partner)
            )

    def stage_w(layer, number):
        own, ghost = own_bufs[layer][number], ghost_bufs[layer][number]
        arrive(marks["own", layer, number, 0], own.at[partner])
        arrive(marks["ghost", layer, number, 0], ghost.at[partner])
        for j in range(1, half):
            source = partner_of(from_peer(j))
            arrive(marks["own2", layer, number, j], own.at[source])
            arrive(marks["ghost2", layer, number, j], ghost.at[source])

    def table_of(layer, number):
        own, ghost = own_bufs[layer][number], ghost_bufs[layer][number]
        blocks = [own[index] for index in range(n_yz)]
        lent = [ghost[index, 0].astype(F32) for index in range(n_yz)]
        lent += [ghost[index, 1].astype(F32) for index in range(n_yz)]
        return jnp.concatenate(blocks + [jnp.concatenate(lent, axis=0).astype(BF16)], axis=0)

    def mixed(layer, number):
        table = table_of(layer, number)
        if number == 0:
            return jnp.dot(table, wv0[layer], preferred_element_type=F32).astype(BF16)
        real, imag = ((wv1, wv2), (wv3, wv4))[number - 1]
        width = table.shape[1] // 2
        stacked = jnp.concatenate([table[:, :width], table[:, width:]], axis=0)
        by_real = jnp.dot(stacked, real[layer], preferred_element_type=F32)
        by_imag = jnp.dot(stacked, imag[layer], preferred_element_type=F32)
        plus = by_real[:table_rows] - by_imag[table_rows:]
        minus = by_imag[:table_rows] + by_real[table_rows:]
        return jnp.concatenate([plus.astype(BF16), minus.astype(BF16)], axis=1)

    def compute(layer, number):
        group = groups[number]
        mix = mixed(layer, number)
        last = layer == LAYERS - 1
        for first in range(0, len(group), 2):
            places = list(range(first, min(first + 2, len(group))))
            columns = slice(places[0] * channels, (places[-1] + 1) * channels)
            gathered = jnp.dot(picks[...], mix[:, columns], preferred_element_type=F32)
            for position, place in enumerate(places):
                part = gathered[:, position * channels : (position + 1) * channels] * radp[layer]
                if last and number == 0 and place == 0:
                    for slot in range(neighb):
                        natural[pl.ds(slot, atoms, stride=neighb), :] = part[
                            slot * atoms : (slot + 1) * atoms
                        ]
                total = part.reshape(neighb, atoms, channels).sum(axis=0)
                lanes = slice(place * channels, (place + 1) * channels)
                fresh = (
                    own_bufs[layer][number][q, :, lanes].astype(F32) + 0.18 * total
                ).astype(BF16)
                if last:
                    unpacked[pl.ds(group[place], atoms, stride=stride), :] = fresh.astype(F32)
                else:
                    own_bufs[layer + 1][number][q, :, lanes] = fresh

    def permuted(store):
        for slot in range(neighb):
            store(
                slice(slot * atoms, (slot + 1) * atoms),
                natural[pl.ds(slot, atoms, stride=neighb), :],
            )

    for number in range(n_groups):
        stage_a(0, number)

    bases = radial_weight.shape[1]
    centers = 1.0 + 0.5 * lax.broadcasted_iota(jnp.int32, (bases, edges), 0).astype(F32)
    basis = jnp.exp(-jnp.square((dist[...] - centers) / 0.5)).T
    row_ids = lax.broadcasted_iota(jnp.int32, (table_rows, edges), 0)
    hot = jnp.where((row_ids == nbr[...]) & (val[...] != 0), 1.0, 0.0).astype(F32)
    scatter[:table_rows, :] = hot
    natural[...] = hot.T

    def keep_picks(rows, values):
        picks[rows, :] = values.astype(BF16)

    permuted(keep_picks)
    for layer in range(LAYERS):
        pre = jnp.dot(basis, radial_weight[layer], precision=HIGHEST, preferred_element_type=F32)
        natural[...] = pre / (1.0 + jnp.exp(-pre))

        def keep_radial(rows, values, layer=layer):
            radp[layer, rows, :] = values

        permuted(keep_radial)

    for number in range(n_groups):
        stage_b(0, number)

    atom_ids = lax.broadcasted_iota(jnp.int32, (atoms, edges), 0)
    edge_ids = lax.broadcasted_iota(jnp.int32, (atoms, edges), 1)
    mine = (edge_ids >= atom_ids * neighb) & (edge_ids < (atom_ids + 1) * neighb)
    scatter[table_rows:, :] = jnp.where(mine, 1.0, 0.0).astype(F32)
    sin_polar = jnp.sin(pol[...])
    part_ids = lax.broadcasted_iota(jnp.int32, (8, edges), 0)
    direction[...] = jnp.where(
        part_ids == 0,
        sin_polar * jnp.cos(azi[...]),
        jnp.where(
            part_ids == 1,
            sin_polar * jnp.sin(azi[...]),
            jnp.where(part_ids == 2, jnp.cos(pol[...]), 0.0),
        ),
    )

    for number in range(n_groups):
        stage_c(0, number)
    for number in range(n_groups):
        stage_d(0, number)
    for copy in weight_copies[0]:
        copy.wait()
    for number in range(n_groups):
        stage_w(0, number)
        compute(0, number)
        lend_rows(1, number)
        stage_a(1, number)
    for copy in weight_copies[1]:
        copy.wait()
    for number in range(n_groups):
        stage_b(1, number)
        stage_c(1, number)

    force_marks = []
    for number in range(n_groups):
        stage_d(1, number)
        stage_w(1, number)
        compute(1, number)
        if number == 0:
            tall = jnp.broadcast_to(readout[...], (8, channels))
            strength = 0.125 * nt_dot(tall, natural[...], HIGHEST)
            parts = nt_dot(direction[...] * strength, scatter[...], HIGHEST)
            own_force = parts[:, table_rows:]
            f_send[...] = -parts[:, :table_rows]
            for index, peer in enumerate(peers):
                force_marks.append(send(f_send, f_recv.at[index], peer))

    for atom in range(atoms):
        out_e[atom] = unpacked[stride * atom : stride * atom + coeffs, :].astype(BF16)

    table_ids = lax.broadcasted_iota(jnp.int32, (atoms, table_rows), 1)
    owner_ids = lax.broadcasted_iota(jnp.int32, (atoms, table_rows), 0)
    pick_own = table_ids == q * atoms + owner_ids
    pick_high = table_ids < 0
    pick_low = table_ids < 0
    for g in range(ghosts):
        pick_high |= (table_ids == own_rows + q * ghosts + g) & (owner_ids == send_high[g])
        pick_low |= (table_ids == own_rows + ghost_rows + q * ghosts + g) & (
            owner_ids == send_low[g]
        )
    choose = jnp.concatenate(
        [jnp.where(pick, 1.0, 0.0).astype(F32) for pick in (pick_own, pick_low, pick_high)], axis=1
    )
    for index, k in enumerate(force_marks):
        arrive(k, f_recv.at[index])
    own_sum = f_send[...]
    for index in range(n_yz - 1):
        own_sum = own_sum + f_recv[index]
    below_sum = f_recv[n_yz - 1]
    above_sum = f_recv[2 * n_yz - 1]
    for index in range(1, n_yz):
        below_sum = below_sum + f_recv[n_yz - 1 + index]
        above_sum = above_sum + f_recv[2 * n_yz - 1 + index]
    gathered = jnp.concatenate([own_sum, below_sum, above_sum], axis=1)
    out_f[...] = (own_force + nt_dot(gathered, choose, HIGHEST))[:3]

    for copy in sends:
        copy.wait_send()


def body(
    n_slab,
    n_yz,
    embeddings,
    neighbours,
    valid,
    azimuth,
    polar,
    distance,
    send_low,
    send_high,
    w_zero,
    w_one_re,
    w_one_im,
    w_two_re,
    w_two_im,
    radial_weight,
    readout,
):
    atoms, coeffs, channels = embeddings.shape
    degrees = math.isqrt(coeffs)
    edges = neighbours.shape[0]
    neighb = edges // atoms
    ghosts = send_low.shape[0]
    stride = (coeffs + 7) // 8 * 8
    groups = slot_groups(degrees)
    table_rows = n_yz * (atoms + 2 * ghosts)
    widths = [len(group) * channels for group in groups]
    weights = (w_zero, w_one_re, w_one_im, w_two_re, w_two_im)
    n_peers = 3 * n_yz - 1
    half = n_yz // 2
    copies = LAYERS * len(groups) * (2 + 2 * half + 2 * (half - 1)) + n_peers
    vmem = pl.BlockSpec(memory_space=pltpu.VMEM)
    smem = pl.BlockSpec(memory_space=pltpu.SMEM)
    hbm = pl.BlockSpec(memory_space=pl.ANY)
    row = lambda array: array.reshape(1, edges)
    scratch = [pltpu.VMEM(weight.shape, BF16) for weight in weights]
    scratch += [
        pltpu.VMEM((atoms * stride, channels), F32),
        pltpu.VMEM((edges, channels), F32),
        pltpu.VMEM((LAYERS, edges, channels), F32),
        pltpu.VMEM((edges, table_rows), BF16),
        pltpu.VMEM((table_rows + atoms, edges), F32),
        pltpu.VMEM((8, edges), F32),
        pltpu.VMEM((8, table_rows), F32),
        pltpu.VMEM((n_peers, 8, table_rows), F32),
    ]
    for _ in range(LAYERS):
        scratch += [pltpu.VMEM((n_yz, atoms, width), BF16) for width in widths]
    for _ in range(LAYERS):
        scratch += [pltpu.VMEM((n_yz, 2, ghosts, width), BF16) for width in widths]
    for _ in range(LAYERS):
        scratch += [pltpu.VMEM((2, ghosts, width), BF16) for width in widths]
    scratch += [
        pltpu.SemaphoreType.DMA((5 * LAYERS,)),
        pltpu.SemaphoreType.DMA((copies,)),
        pltpu.SemaphoreType.DMA((copies,)),
    ]
    return pl.pallas_call(
        functools.partial(
            kernel, n_slab, n_yz, atoms, coeffs, stride, channels, ghosts, neighb, groups
        ),
        out_shape=(
            jax.ShapeDtypeStruct(embeddings.shape, BF16),
            jax.ShapeDtypeStruct((3, atoms), F32),
        ),
        in_specs=[vmem] * 6 + [smem] * 2 + [hbm] * 5 + [vmem] * 2,
        out_specs=(vmem, vmem),
        scratch_shapes=scratch,
        compiler_params=pltpu.CompilerParams(collective_id=0, has_side_effects=True),
    )(
        embeddings,
        row(neighbours),
        row(valid),
        row(azimuth),
        row(polar),
        row(distance),
        send_low,
        send_high,
        *weights,
        radial_weight,
        readout.reshape(1, channels),
    )


def solution(mesh):
    both = ("slab", "yz")
    in_specs = (P(both, None, None),) + (P(both),) * 7 + (P(),) * 7
    out_specs = (P(both, None, None), P(None, both))
    return jax.shard_map(
        functools.partial(body, mesh.shape["slab"], mesh.shape["yz"]),
        mesh=mesh,
        in_specs=in_specs,
        out_specs=out_specs,
        check_vma=False,
    )
```

```python
import functools
import math

import jax
import jax.numpy as jnp
from jax import lax
from jax.experimental import pallas as pl
from jax.experimental.pallas import tpu as pltpu
from jax.sharding import PartitionSpec as P

LAYERS = 2
MESH = pl.DeviceIdType.MESH
HIGHEST = lax.Precision.HIGHEST
F32 = jnp.float32
BF16 = jnp.bfloat16


def slot_index(degree, order):
    return degree * degree + degree + order


def slot_groups(degrees):
    groups = [[slot_index(degree, 0) for degree in range(degrees)]]
    for order in (1, 2):
        groups.append(
            [slot_index(degree, order) for degree in range(order, degrees)]
            + [slot_index(degree, -order) for degree in range(order, degrees)]
        )
    return groups


def nt_dot(left, right, precision=None):
    return lax.dot_general(
        left, right, (((1,), (1,)), ((), ())), precision=precision, preferred_element_type=F32
    )


def kernel(
    n_slab,
    n_yz,
    atoms,
    coeffs,
    channels,
    ghosts,
    neighb,
    groups,
    emb,
    nbr,
    val,
    azi,
    pol,
    dist,
    send_low,
    send_high,
    w_hbm0,
    w_hbm1,
    w_hbm2,
    w_hbm3,
    w_hbm4,
    radial_weight,
    readout,
    out_e,
    out_f,
    wv0,
    wv1,
    wv2,
    wv3,
    wv4,
    natural,
    radp,
    picks,
    scatter,
    direction,
    f_send,
    f_recv,
    *rest,
):
    n_groups = len(groups)
    own_bufs = [rest[layer * n_groups : (layer + 1) * n_groups] for layer in range(LAYERS)]
    rest = rest[LAYERS * n_groups :]
    ghost_bufs = [rest[layer * n_groups : (layer + 1) * n_groups] for layer in range(LAYERS)]
    rest = rest[LAYERS * n_groups :]
    lend_bufs = [rest[layer * n_groups : (layer + 1) * n_groups] for layer in range(LAYERS)]
    rest = rest[LAYERS * n_groups :]
    weight_sem, send_sem, recv_sem = rest

    edges = atoms * neighb
    own_rows = n_yz * atoms
    ghost_rows = n_yz * ghosts
    table_rows = own_rows + 2 * ghost_rows
    half = n_yz // 2

    slab = lax.axis_index("slab")
    q = lax.axis_index("yz")
    above = lax.rem(slab + 1, n_slab)
    below = lax.rem(slab + n_slab - 1, n_slab)
    core = lax.rem(q, 2)
    row = q // 2
    partner = q + 1 - 2 * core

    def to_peer(j):
        return lax.rem(row + j, half) * 2 + core

    def from_peer(j):
        return lax.rem(row + half - j, half) * 2 + core

    def partner_of(index):
        return index + 1 - 2 * lax.rem(index, 2)

    weight_pairs = ((w_hbm0, wv0), (w_hbm1, wv1), (w_hbm2, wv2), (w_hbm3, wv3), (w_hbm4, wv4))
    weight_copies = [
        [
            pltpu.make_async_copy(
                source.at[layer], target.at[layer], weight_sem.at[layer * 5 + number]
            )
            for number, (source, target) in enumerate(weight_pairs)
        ]
        for layer in range(LAYERS)
    ]
    for layer in range(LAYERS):
        for copy in weight_copies[layer]:
            copy.start()

    barrier = pltpu.get_barrier_semaphore()
    peers = [(slab, lax.rem(q + j, n_yz)) for j in range(1, n_yz)]
    peers += [(above, lax.rem(q + j, n_yz)) for j in range(n_yz)]
    peers += [(below, lax.rem(q + j, n_yz)) for j in range(n_yz)]
    for peer in peers:
        pl.semaphore_signal(barrier, inc=1, device_id=peer, device_id_type=MESH)

    lend_row = lax.broadcasted_iota(jnp.int32, (2 * ghosts, atoms), 0)
    lend_col = lax.broadcasted_iota(jnp.int32, (2 * ghosts, atoms), 1)
    wanted = jnp.zeros((2 * ghosts, atoms), jnp.int32)
    for g in range(ghosts):
        wanted = jnp.where(lend_row == g, send_high[g], wanted)
        wanted = jnp.where(lend_row == ghosts + g, send_low[g], wanted)
    lend = (wanted == lend_col).astype(F32).astype(BF16)

    def lend_rows(layer, number):
        rows = jnp.dot(lend, own_bufs[layer][number][q], preferred_element_type=F32)
        lend_bufs[layer][number][0] = rows[:ghosts].astype(BF16)
        lend_bufs[layer][number][1] = rows[ghosts:].astype(BF16)

    for number, group in enumerate(groups):
        for place, slot in enumerate(group):
            own_bufs[0][number][q, :, place * channels : (place + 1) * channels] = emb[slot]
        lend_rows(0, number)

    pl.semaphore_wait(barrier, len(peers))

    sends = []
    count = [0]

    def send(source, target, device):
        k = count[0]
        count[0] += 1
        copy = pltpu.make_async_remote_copy(
            src_ref=source,
            dst_ref=target,
            send_sem=send_sem.at[k],
            recv_sem=recv_sem.at[k],
            device_id=device,
            device_id_type=MESH,
        )
        copy.start()
        sends.append(copy)
        return k

    def arrive(k, target):
        pltpu.make_async_remote_copy(
            src_ref=target,
            dst_ref=target,
            send_sem=send_sem.at[k],
            recv_sem=recv_sem.at[k],
            device_id=(slab, partner),
            device_id_type=MESH,
        ).wait_recv()

    marks = {}

    def stage_a(layer, number):
        own, ghost, lent = (
            own_bufs[layer][number],
            ghost_bufs[layer][number],
            lend_bufs[layer][number],
        )
        marks["up", layer, number] = send(lent.at[0], ghost.at[q, 0], (above, q))
        marks["down", layer, number] = send(lent.at[1], ghost.at[q, 1], (below, q))
        for j in range(1, half):
            marks["own", layer, number, j] = send(own.at[q], own.at[q], (slab, to_peer(j)))
        marks["own", layer, number, 0] = send(own.at[q], own.at[q], (slab, partner))

    def stage_b(layer, number):
        own = own_bufs[layer][number]
        for j in range(1, half):
            source = from_peer(j)
            arrive(marks["own", layer, number, j], own.at[source])
            marks["own2", layer, number, j] = send(
                own.at[source], own.at[source], (slab, partner)
            )

    def stage_c(layer, number):
        ghost = ghost_bufs[layer][number]
        arrive(marks["up", layer, number], ghost.at[q, 0])
        arrive(marks["down", layer, number], ghost.at[q, 1])
        for j in range(1, half):
            marks["ghost", layer, number, j] = send(
                ghost.at[q], ghost.at[q], (slab, to_peer(j))
            )
        marks["ghost", layer, number, 0] = send(ghost.at[q], ghost.at[q], (slab, partner))

    def stage_d(layer, number):
        ghost = ghost_bufs[layer][number]
        for j in range(1, half):
            source = from_peer(j)
            arrive(marks["ghost", layer, number, j], ghost.at[source])
            marks["ghost2", layer, number, j] = send(
                ghost.at[source], ghost.at[source], (slab, partner)
            )

    def stage_w(layer, number):
        own, ghost = own_bufs[layer][number], ghost_bufs[layer][number]
        arrive(marks["own", layer, number, 0], own.at[partner])
        arrive(marks["ghost", layer, number, 0], ghost.at[partner])
        for j in range(1, half):
            source = partner_of(from_peer(j))
            arrive(marks["own2", layer, number, j], own.at[source])
            arrive(marks["ghost2", layer, number, j], ghost.at[source])

    def table_of(layer, number):
        own, ghost = own_bufs[layer][number], ghost_bufs[layer][number]
        blocks = [own[index] for index in range(n_yz)]
        lent = [ghost[index, 0].astype(F32) for index in range(n_yz)]
        lent += [ghost[index, 1].astype(F32) for index in range(n_yz)]
        return jnp.concatenate(blocks + [jnp.concatenate(lent, axis=0).astype(BF16)], axis=0)

    def mixed(layer, number):
        table = table_of(layer, number)
        if number == 0:
            return jnp.dot(table, wv0[layer], preferred_element_type=F32).astype(BF16)
        real, imag = ((wv1, wv2), (wv3, wv4))[number - 1]
        width = table.shape[1] // 2
        stacked = jnp.concatenate([table[:, :width], table[:, width:]], axis=0)
        by_real = jnp.dot(stacked, real[layer], preferred_element_type=F32)
        by_imag = jnp.dot(stacked, imag[layer], preferred_element_type=F32)
        plus = by_real[:table_rows] - by_imag[table_rows:]
        minus = by_imag[:table_rows] + by_real[table_rows:]
        return jnp.concatenate([plus.astype(BF16), minus.astype(BF16)], axis=1)

    def compute(layer, number):
        group = groups[number]
        mix = mixed(layer, number)
        last = layer == LAYERS - 1
        for first in range(0, len(group), 2):
            places = list(range(first, min(first + 2, len(group))))
            columns = slice(places[0] * channels, (places[-1] + 1) * channels)
            gathered = jnp.dot(picks[...], mix[:, columns], preferred_element_type=F32)
            for position, place in enumerate(places):
                part = gathered[:, position * channels : (position + 1) * channels] * radp[layer]
                if last and number == 0 and place == 0:
                    for slot in range(neighb):
                        natural[pl.ds(slot, atoms, stride=neighb), :] = part[
                            slot * atoms : (slot + 1) * atoms
                        ]
                total = part.reshape(neighb, atoms, channels).sum(axis=0)
                lanes = slice(place * channels, (place + 1) * channels)
                fresh = (
                    own_bufs[layer][number][q, :, lanes].astype(F32) + 0.18 * total
                ).astype(BF16)
                if last:
                    out_e[group[place]] = fresh
                else:
                    own_bufs[layer + 1][number][q, :, lanes] = fresh

    def permuted(store):
        for slot in range(neighb):
            store(
                slice(slot * atoms, (slot + 1) * atoms),
                natural[pl.ds(slot, atoms, stride=neighb), :],
            )

    for number in range(n_groups):
        stage_a(0, number)

    bases = radial_weight.shape[1]
    centers = 1.0 + 0.5 * lax.broadcasted_iota(jnp.int32, (bases, edges), 0).astype(F32)
    basis = jnp.exp(-jnp.square((dist[...] - centers) / 0.5)).T
    row_ids = lax.broadcasted_iota(jnp.int32, (table_rows, edges), 0)
    hot = jnp.where((row_ids == nbr[...]) & (val[...] != 0), 1.0, 0.0).astype(F32)
    scatter[:table_rows, :] = hot
    natural[...] = hot.T

    def keep_picks(rows, values):
        picks[rows, :] = values.astype(BF16)

    permuted(keep_picks)
    for layer in range(LAYERS):
        pre = jnp.dot(basis, radial_weight[layer], precision=HIGHEST, preferred_element_type=F32)
        natural[...] = pre / (1.0 + jnp.exp(-pre))

        def keep_radial(rows, values, layer=layer):
            radp[layer, rows, :] = values

        permuted(keep_radial)

    for number in range(n_groups):
        stage_b(0, number)

    atom_ids = lax.broadcasted_iota(jnp.int32, (atoms, edges), 0)
    edge_ids = lax.broadcasted_iota(jnp.int32, (atoms, edges), 1)
    mine = (edge_ids >= atom_ids * neighb) & (edge_ids < (atom_ids + 1) * neighb)
    scatter[table_rows:, :] = jnp.where(mine, 1.0, 0.0).astype(F32)
    sin_polar = jnp.sin(pol[...])
    part_ids = lax.broadcasted_iota(jnp.int32, (8, edges), 0)
    direction[...] = jnp.where(
        part_ids == 0,
        sin_polar * jnp.cos(azi[...]),
        jnp.where(
            part_ids == 1,
            sin_polar * jnp.sin(azi[...]),
            jnp.where(part_ids == 2, jnp.cos(pol[...]), 0.0),
        ),
    )

    for number in range(n_groups):
        stage_c(0, number)
    for number in range(n_groups):
        stage_d(0, number)
    for copy in weight_copies[0]:
        copy.wait()
    for number in range(n_groups):
        stage_w(0, number)
        compute(0, number)
        lend_rows(1, number)
        stage_a(1, number)
    for copy in weight_copies[1]:
        copy.wait()
    for number in range(n_groups):
        stage_b(1, number)
        stage_c(1, number)

    force_marks = []
    for number in range(n_groups):
        stage_d(1, number)
        stage_w(1, number)
        compute(1, number)
        if number == 0:
            tall = jnp.broadcast_to(readout[...], (8, channels))
            strength = 0.125 * nt_dot(tall, natural[...], HIGHEST)
            parts = nt_dot(direction[...] * strength, scatter[...], HIGHEST)
            own_force = parts[:, table_rows:]
            f_send[...] = -parts[:, :table_rows]
            for index, peer in enumerate(peers):
                force_marks.append(send(f_send, f_recv.at[index], peer))

    for slot in range(coeffs):
        if not any(slot in group for group in groups):
            out_e[slot] = emb[slot]

    table_ids = lax.broadcasted_iota(jnp.int32, (atoms, table_rows), 1)
    owner_ids = lax.broadcasted_iota(jnp.int32, (atoms, table_rows), 0)
    pick_own = table_ids == q * atoms + owner_ids
    pick_high = table_ids < 0
    pick_low = table_ids < 0
    for g in range(ghosts):
        pick_high |= (table_ids == own_rows + q * ghosts + g) & (owner_ids == send_high[g])
        pick_low |= (table_ids == own_rows + ghost_rows + q * ghosts + g) & (
            owner_ids == send_low[g]
        )
    choose = jnp.concatenate(
        [jnp.where(pick, 1.0, 0.0).astype(F32) for pick in (pick_own, pick_low, pick_high)], axis=1
    )
    for index, k in enumerate(force_marks):
        arrive(k, f_recv.at[index])
    own_sum = f_send[...]
    for index in range(n_yz - 1):
        own_sum = own_sum + f_recv[index]
    below_sum = f_recv[n_yz - 1]
    above_sum = f_recv[2 * n_yz - 1]
    for index in range(1, n_yz):
        below_sum = below_sum + f_recv[n_yz - 1 + index]
        above_sum = above_sum + f_recv[2 * n_yz - 1 + index]
    gathered = jnp.concatenate([own_sum, below_sum, above_sum], axis=1)
    out_f[...] = (own_force + nt_dot(gathered, choose, HIGHEST))[:3]

    for copy in sends:
        copy.wait_send()


def body(
    n_slab,
    n_yz,
    embeddings,
    neighbours,
    valid,
    azimuth,
    polar,
    distance,
    send_low,
    send_high,
    w_zero,
    w_one_re,
    w_one_im,
    w_two_re,
    w_two_im,
    radial_weight,
    readout,
):
    atoms, coeffs, channels = embeddings.shape
    degrees = math.isqrt(coeffs)
    edges = neighbours.shape[0]
    neighb = edges // atoms
    ghosts = send_low.shape[0]
    groups = slot_groups(degrees)
    table_rows = n_yz * (atoms + 2 * ghosts)
    widths = [len(group) * channels for group in groups]
    weights = (w_zero, w_one_re, w_one_im, w_two_re, w_two_im)
    n_peers = 3 * n_yz - 1
    half = n_yz // 2
    copies = LAYERS * len(groups) * (2 + 2 * half + 2 * (half - 1)) + n_peers
    vmem = pl.BlockSpec(memory_space=pltpu.VMEM)
    smem = pl.BlockSpec(memory_space=pltpu.SMEM)
    hbm = pl.BlockSpec(memory_space=pl.ANY)
    row = lambda array: array.reshape(1, edges)
    scratch = [pltpu.VMEM(weight.shape, BF16) for weight in weights]
    scratch += [
        pltpu.VMEM((edges, channels), F32),
        pltpu.VMEM((LAYERS, edges, channels), F32),
        pltpu.VMEM((edges, table_rows), BF16),
        pltpu.VMEM((table_rows + atoms, edges), F32),
        pltpu.VMEM((8, edges), F32),
        pltpu.VMEM((8, table_rows), F32),
        pltpu.VMEM((n_peers, 8, table_rows), F32),
    ]
    for _ in range(LAYERS):
        scratch += [pltpu.VMEM((n_yz, atoms, width), BF16) for width in widths]
    for _ in range(LAYERS):
        scratch += [pltpu.VMEM((n_yz, 2, ghosts, width), BF16) for width in widths]
    for _ in range(LAYERS):
        scratch += [pltpu.VMEM((2, ghosts, width), BF16) for width in widths]
    scratch += [
        pltpu.SemaphoreType.DMA((5 * LAYERS,)),
        pltpu.SemaphoreType.DMA((copies,)),
        pltpu.SemaphoreType.DMA((copies,)),
    ]
    updated, forces = pl.pallas_call(
        functools.partial(
            kernel, n_slab, n_yz, atoms, coeffs, channels, ghosts, neighb, groups
        ),
        out_shape=(
            jax.ShapeDtypeStruct((coeffs, atoms, channels), BF16),
            jax.ShapeDtypeStruct((3, atoms), F32),
        ),
        in_specs=[vmem] * 6 + [smem] * 2 + [hbm] * 5 + [vmem] * 2,
        out_specs=(vmem, vmem),
        scratch_shapes=scratch,
        compiler_params=pltpu.CompilerParams(collective_id=0, has_side_effects=True),
    )(
        jnp.transpose(embeddings, (1, 0, 2)),
        row(neighbours),
        row(valid),
        row(azimuth),
        row(polar),
        row(distance),
        send_low,
        send_high,
        *weights,
        radial_weight,
        readout.reshape(1, channels),
    )
    return (jnp.transpose(updated, (1, 0, 2)), forces)


def solution(mesh):
    both = ("slab", "yz")
    in_specs = (P(both, None, None),) + (P(both),) * 7 + (P(),) * 7
    out_specs = (P(both, None, None), P(None, both))
    return jax.shard_map(
        functools.partial(body, mesh.shape["slab"], mesh.shape["yz"]),
        mesh=mesh,
        in_specs=in_specs,
        out_specs=out_specs,
        check_vma=False,
    )
```

```python
import functools
import math

import jax
import jax.numpy as jnp
from jax import lax
from jax.experimental import pallas as pl
from jax.experimental.pallas import tpu as pltpu
from jax.sharding import PartitionSpec as P

LAYERS = 2
MESH = pl.DeviceIdType.MESH
HIGHEST = lax.Precision.HIGHEST
F32 = jnp.float32
BF16 = jnp.bfloat16


def slot_index(degree, order):
    return degree * degree + degree + order


def slot_groups(degrees):
    groups = [[slot_index(degree, 0) for degree in range(degrees)]]
    for order in (1, 2):
        groups.append(
            [slot_index(degree, order) for degree in range(order, degrees)]
            + [slot_index(degree, -order) for degree in range(order, degrees)]
        )
    return groups


def nt_dot(left, right, precision=None):
    return lax.dot_general(
        left, right, (((1,), (1,)), ((), ())), precision=precision, preferred_element_type=F32
    )


def thirds(values):
    head = values.astype(BF16).astype(F32)
    mid = (values - head).astype(BF16).astype(F32)
    return head, mid, values - head - mid


def thirds_dot(values, exact):
    rows = jnp.concatenate(thirds(values), axis=0).astype(BF16)
    total = nt_dot(rows, exact)
    count = values.shape[0]
    return total[:count] + (total[count : 2 * count] + total[2 * count :])


def kernel(
    n_slab,
    n_yz,
    atoms,
    coeffs,
    channels,
    ghosts,
    neighb,
    groups,
    emb,
    nbr,
    val,
    azi,
    pol,
    dist,
    send_low,
    send_high,
    w_hbm0,
    w_hbm1,
    w_hbm2,
    w_hbm3,
    w_hbm4,
    radial_weight,
    readout,
    out_e,
    out_f,
    wv0,
    wv1,
    wv2,
    wv3,
    wv4,
    natural,
    radp,
    picks,
    scatter,
    direction,
    chooser,
    fresh_e,
    f_send,
    f_recv,
    *rest,
):
    n_groups = len(groups)
    own_bufs = [rest[layer * n_groups : (layer + 1) * n_groups] for layer in range(LAYERS)]
    rest = rest[LAYERS * n_groups :]
    ghost_bufs = [rest[layer * n_groups : (layer + 1) * n_groups] for layer in range(LAYERS)]
    rest = rest[LAYERS * n_groups :]
    lend_bufs = [rest[layer * n_groups : (layer + 1) * n_groups] for layer in range(LAYERS)]
    rest = rest[LAYERS * n_groups :]
    weight_sem, out_sem, send_sem, recv_sem = rest

    edges = atoms * neighb
    own_rows = n_yz * atoms
    ghost_rows = n_yz * ghosts
    table_rows = own_rows + 2 * ghost_rows
    half = n_yz // 2

    slab = lax.axis_index("slab")
    q = lax.axis_index("yz")
    above = lax.rem(slab + 1, n_slab)
    below = lax.rem(slab + n_slab - 1, n_slab)
    core = lax.rem(q, 2)
    row = q // 2
    partner = q + 1 - 2 * core

    def to_peer(j):
        return lax.rem(row + j, half) * 2 + core

    def from_peer(j):
        return lax.rem(row + half - j, half) * 2 + core

    def partner_of(index):
        return index + 1 - 2 * lax.rem(index, 2)

    weight_pairs = ((w_hbm0, wv0), (w_hbm1, wv1), (w_hbm2, wv2), (w_hbm3, wv3), (w_hbm4, wv4))
    weight_copies = [
        [
            pltpu.make_async_copy(
                source.at[layer], target.at[layer], weight_sem.at[layer * 5 + number]
            )
            for number, (source, target) in enumerate(weight_pairs)
        ]
        for layer in range(LAYERS)
    ]
    for layer in range(LAYERS):
        for copy in weight_copies[layer]:
            copy.start()

    barrier = pltpu.get_barrier_semaphore()
    peers = [(slab, lax.rem(q + j, n_yz)) for j in range(1, n_yz)]
    peers += [(above, lax.rem(q + j, n_yz)) for j in range(n_yz)]
    peers += [(below, lax.rem(q + j, n_yz)) for j in range(n_yz)]
    for peer in peers:
        pl.semaphore_signal(barrier, inc=1, device_id=peer, device_id_type=MESH)

    lend_row = lax.broadcasted_iota(jnp.int32, (2 * ghosts, atoms), 0)
    lend_col = lax.broadcasted_iota(jnp.int32, (2 * ghosts, atoms), 1)
    wanted = jnp.zeros((2 * ghosts, atoms), jnp.int32)
    for g in range(ghosts):
        wanted = jnp.where(lend_row == g, send_high[g], wanted)
        wanted = jnp.where(lend_row == ghosts + g, send_low[g], wanted)
    lend = (wanted == lend_col).astype(F32).astype(BF16)

    def lend_rows(layer, number):
        rows = jnp.dot(lend, own_bufs[layer][number][q], preferred_element_type=F32)
        lend_bufs[layer][number][0] = rows[:ghosts].astype(BF16)
        lend_bufs[layer][number][1] = rows[ghosts:].astype(BF16)

    for number, group in enumerate(groups):
        for place, slot in enumerate(group):
            own_bufs[0][number][q, :, place * channels : (place + 1) * channels] = emb[slot]
        lend_rows(0, number)

    pl.semaphore_wait(barrier, len(peers))

    sends = []
    count = [0]

    def send(source, target, device):
        k = count[0]
        count[0] += 1
        copy = pltpu.make_async_remote_copy(
            src_ref=source,
            dst_ref=target,
            send_sem=send_sem.at[k],
            recv_sem=recv_sem.at[k],
            device_id=device,
            device_id_type=MESH,
        )
        copy.start()
        sends.append(copy)
        return k

    def arrive(k, target):
        pltpu.make_async_remote_copy(
            src_ref=target,
            dst_ref=target,
            send_sem=send_sem.at[k],
            recv_sem=recv_sem.at[k],
            device_id=(slab, partner),
            device_id_type=MESH,
        ).wait_recv()

    marks = {}

    def stage_a(layer, number):
        own, ghost, lent = (
            own_bufs[layer][number],
            ghost_bufs[layer][number],
            lend_bufs[layer][number],
        )
        marks["up", layer, number] = send(lent.at[0], ghost.at[q, 0], (above, q))
        marks["down", layer, number] = send(lent.at[1], ghost.at[q, 1], (below, q))
        for j in range(1, half):
            marks["own", layer, number, j] = send(own.at[q], own.at[q], (slab, to_peer(j)))
        marks["own", layer, number, 0] = send(own.at[q], own.at[q], (slab, partner))

    def stage_b(layer, number):
        own = own_bufs[layer][number]
        for j in range(1, half):
            source = from_peer(j)
            arrive(marks["own", layer, number, j], own.at[source])
            marks["own2", layer, number, j] = send(
                own.at[source], own.at[source], (slab, partner)
            )

    def stage_c(layer, number):
        ghost = ghost_bufs[layer][number]
        arrive(marks["up", layer, number], ghost.at[q, 0])
        arrive(marks["down", layer, number], ghost.at[q, 1])
        for j in range(1, half):
            marks["ghost", layer, number, j] = send(
                ghost.at[q], ghost.at[q], (slab, to_peer(j))
            )
        marks["ghost", layer, number, 0] = send(ghost.at[q], ghost.at[q], (slab, partner))

    def stage_d(layer, number):
        ghost = ghost_bufs[layer][number]
        for j in range(1, half):
            source = from_peer(j)
            arrive(marks["ghost", layer, number, j], ghost.at[source])
            marks["ghost2", layer, number, j] = send(
                ghost.at[source], ghost.at[source], (slab, partner)
            )

    def stage_w(layer, number):
        own, ghost = own_bufs[layer][number], ghost_bufs[layer][number]
        arrive(marks["own", layer, number, 0], own.at[partner])
        arrive(marks["ghost", layer, number, 0], ghost.at[partner])
        for j in range(1, half):
            source = partner_of(from_peer(j))
            arrive(marks["own2", layer, number, j], own.at[source])
            arrive(marks["ghost2", layer, number, j], ghost.at[source])

    def table_of(layer, number):
        own, ghost = own_bufs[layer][number], ghost_bufs[layer][number]
        blocks = [own[index] for index in range(n_yz)]
        lent = [ghost[index, 0].astype(F32) for index in range(n_yz)]
        lent += [ghost[index, 1].astype(F32) for index in range(n_yz)]
        return jnp.concatenate(blocks + [jnp.concatenate(lent, axis=0).astype(BF16)], axis=0)

    def mixed(layer, number):
        table = table_of(layer, number)
        if number == 0:
            return jnp.dot(table, wv0[layer], preferred_element_type=F32).astype(BF16)
        real, imag = ((wv1, wv2), (wv3, wv4))[number - 1]
        width = table.shape[1] // 2
        stacked = jnp.concatenate([table[:, :width], table[:, width:]], axis=0)
        by_real = jnp.dot(stacked, real[layer], preferred_element_type=F32)
        by_imag = jnp.dot(stacked, imag[layer], preferred_element_type=F32)
        plus = by_real[:table_rows] - by_imag[table_rows:]
        minus = by_imag[:table_rows] + by_real[table_rows:]
        return jnp.concatenate([plus.astype(BF16), minus.astype(BF16)], axis=1)

    def compute(layer, number):
        group = groups[number]
        mix = mixed(layer, number)
        last = layer == LAYERS - 1
        for first in range(0, len(group), 2):
            places = list(range(first, min(first + 2, len(group))))
            columns = slice(places[0] * channels, (places[-1] + 1) * channels)
            gathered = jnp.dot(picks[...], mix[:, columns], preferred_element_type=F32)
            for position, place in enumerate(places):
                part = gathered[:, position * channels : (position + 1) * channels] * radp[layer]
                if last and number == 0 and place == 0:
                    for slot in range(neighb):
                        natural[pl.ds(slot, atoms, stride=neighb), :] = part[
                            slot * atoms : (slot + 1) * atoms
                        ]
                total = part.reshape(neighb, atoms, channels).sum(axis=0)
                lanes = slice(place * channels, (place + 1) * channels)
                fresh = (
                    own_bufs[layer][number][q, :, lanes].astype(F32) + 0.18 * total
                ).astype(BF16)
                if last:
                    fresh_e[group[place]] = fresh
                else:
                    own_bufs[layer + 1][number][q, :, lanes] = fresh

    def permuted(store):
        for slot in range(neighb):
            store(
                slice(slot * atoms, (slot + 1) * atoms),
                natural[pl.ds(slot, atoms, stride=neighb), :],
            )

    for number in range(n_groups):
        stage_a(0, number)

    bases = radial_weight.shape[1]
    centers = 1.0 + 0.5 * lax.broadcasted_iota(jnp.int32, (bases, edges), 0).astype(F32)
    basis = jnp.exp(-jnp.square((dist[...] - centers) / 0.5)).T
    row_ids = lax.broadcasted_iota(jnp.int32, (table_rows, edges), 0)
    hot = jnp.where((row_ids == nbr[...]) & (val[...] != 0), 1.0, 0.0).astype(F32)
    scatter[:table_rows, :] = hot.astype(BF16)
    natural[...] = hot.T

    def keep_picks(rows, values):
        picks[rows, :] = values.astype(BF16)

    permuted(keep_picks)
    for layer in range(LAYERS):
        pre = jnp.dot(basis, radial_weight[layer], precision=HIGHEST, preferred_element_type=F32)
        natural[...] = pre / (1.0 + jnp.exp(-pre))

        def keep_radial(rows, values, layer=layer):
            radp[layer, rows, :] = values

        permuted(keep_radial)

    for number in range(n_groups):
        stage_b(0, number)

    atom_ids = lax.broadcasted_iota(jnp.int32, (atoms, edges), 0)
    edge_ids = lax.broadcasted_iota(jnp.int32, (atoms, edges), 1)
    mine = (edge_ids >= atom_ids * neighb) & (edge_ids < (atom_ids + 1) * neighb)
    scatter[table_rows:, :] = jnp.where(mine, 1.0, 0.0).astype(F32).astype(BF16)
    sin_polar = jnp.sin(pol[...])
    part_ids = lax.broadcasted_iota(jnp.int32, (8, edges), 0)
    direction[...] = jnp.where(
        part_ids == 0,
        sin_polar * jnp.cos(azi[...]),
        jnp.where(
            part_ids == 1,
            sin_polar * jnp.sin(azi[...]),
            jnp.where(part_ids == 2, jnp.cos(pol[...]), 0.0),
        ),
    )

    table_ids = lax.broadcasted_iota(jnp.int32, (atoms, table_rows), 1)
    owner_ids = lax.broadcasted_iota(jnp.int32, (atoms, table_rows), 0)
    pick = table_ids == q * atoms + owner_ids
    for g in range(ghosts):
        pick |= (table_ids == own_rows + q * ghosts + g) & (owner_ids == send_high[g])
        pick |= (table_ids == own_rows + ghost_rows + q * ghosts + g) & (
            owner_ids == send_low[g]
        )
    chooser[...] = jnp.where(pick, 1.0, 0.0).astype(F32).astype(BF16)

    out_copies = []

    def write_out(source, slots):
        for slot in slots:
            copy = pltpu.make_async_copy(source.at[slot], out_e.at[slot], out_sem.at[slot])
            copy.start()
            out_copies.append(copy)

    used = {slot for group in groups for slot in group}
    write_out(emb, [slot for slot in range(coeffs) if slot not in used])

    for number in range(n_groups):
        stage_c(0, number)
    for number in range(n_groups):
        stage_d(0, number)
    for copy in weight_copies[0]:
        copy.wait()
    for number in range(n_groups):
        stage_w(0, number)
        compute(0, number)
        lend_rows(1, number)
        stage_a(1, number)
    for copy in weight_copies[1]:
        copy.wait()
    for number in range(n_groups):
        stage_b(1, number)
        stage_c(1, number)

    force_marks = []
    for number in range(n_groups):
        stage_d(1, number)
    for number in range(n_groups):
        stage_w(1, number)
        compute(1, number)
        write_out(fresh_e, groups[number])
        if number == 0:
            tall = jnp.broadcast_to(readout[...], (8, channels))
            tall_head, tall_mid, tall_tail = thirds(tall)
            tall_rows = jnp.concatenate([tall_head, tall_mid, tall_tail], axis=0).astype(BF16)
            scalar_head, scalar_mid, scalar_tail = thirds(natural[...])
            total = nt_dot(tall_rows, scalar_head.astype(BF16))
            total += nt_dot(tall_rows, scalar_mid.astype(BF16))
            total += nt_dot(tall_rows, scalar_tail.astype(BF16))
            strength = 0.125 * (total[:8] + (total[8:16] + total[16:24]))
            parts = thirds_dot(direction[...] * strength, scatter[...])
            own_force = parts[:, table_rows:]
            f_send[...] = -parts[:, :table_rows]
            for index, peer in enumerate(peers):
                force_marks.append(send(f_send, f_recv.at[index], peer))

    for index, k in enumerate(force_marks):
        arrive(k, f_recv.at[index])
    own_sum = f_send[...]
    for index in range(n_yz - 1):
        own_sum = own_sum + f_recv[index]
    below_sum = f_recv[n_yz - 1]
    above_sum = f_recv[2 * n_yz - 1]
    for index in range(1, n_yz):
        below_sum = below_sum + f_recv[n_yz - 1 + index]
        above_sum = above_sum + f_recv[2 * n_yz - 1 + index]
    lane = lax.broadcasted_iota(jnp.int32, (8, table_rows), 1)
    returned = jnp.where(
        lane < own_rows,
        own_sum,
        jnp.where(lane < own_rows + ghost_rows, above_sum, below_sum),
    )
    out_f[...] = (own_force + thirds_dot(returned, chooser[...]))[:3]

    for copy in out_copies:
        copy.wait()
    for copy in sends:
        copy.wait_send()


def hand_over(rows, forces, rows_out, forces_out):
    rows_out[...] = rows[...]
    forces_out[...] = forces[...]


def body(
    n_slab,
    n_yz,
    embeddings,
    neighbours,
    valid,
    azimuth,
    polar,
    distance,
    send_low,
    send_high,
    w_zero,
    w_one_re,
    w_one_im,
    w_two_re,
    w_two_im,
    radial_weight,
    readout,
):
    atoms, coeffs, channels = embeddings.shape
    degrees = math.isqrt(coeffs)
    edges = neighbours.shape[0]
    neighb = edges // atoms
    ghosts = send_low.shape[0]
    groups = slot_groups(degrees)
    table_rows = n_yz * (atoms + 2 * ghosts)
    widths = [len(group) * channels for group in groups]
    weights = (w_zero, w_one_re, w_one_im, w_two_re, w_two_im)
    n_peers = 3 * n_yz - 1
    half = n_yz // 2
    copies = LAYERS * len(groups) * (2 + 2 * half + 2 * (half - 1)) + n_peers
    vmem = pl.BlockSpec(memory_space=pltpu.VMEM)
    smem = pl.BlockSpec(memory_space=pltpu.SMEM)
    hbm = pl.BlockSpec(memory_space=pl.ANY)
    row = lambda array: array.reshape(1, edges)
    scratch = [pltpu.VMEM(weight.shape, BF16) for weight in weights]
    scratch += [
        pltpu.VMEM((edges, channels), F32),
        pltpu.VMEM((LAYERS, edges, channels), F32),
        pltpu.VMEM((edges, table_rows), BF16),
        pltpu.VMEM((table_rows + atoms, edges), BF16),
        pltpu.VMEM((8, edges), F32),
        pltpu.VMEM((atoms, table_rows), BF16),
        pltpu.VMEM((coeffs, atoms, channels), BF16),
        pltpu.VMEM((8, table_rows), F32),
        pltpu.VMEM((n_peers, 8, table_rows), F32),
    ]
    for _ in range(LAYERS):
        scratch += [pltpu.VMEM((n_yz, atoms, width), BF16) for width in widths]
    for _ in range(LAYERS):
        scratch += [pltpu.VMEM((n_yz, 2, ghosts, width), BF16) for width in widths]
    for _ in range(LAYERS):
        scratch += [pltpu.VMEM((2, ghosts, width), BF16) for width in widths]
    scratch += [
        pltpu.SemaphoreType.DMA((5 * LAYERS,)),
        pltpu.SemaphoreType.DMA((coeffs,)),
        pltpu.SemaphoreType.DMA((copies,)),
        pltpu.SemaphoreType.DMA((copies,)),
    ]
    updated, forces = pl.pallas_call(
        functools.partial(
            kernel, n_slab, n_yz, atoms, coeffs, channels, ghosts, neighb, groups
        ),
        out_shape=(
            jax.ShapeDtypeStruct((coeffs, atoms, channels), BF16),
            jax.ShapeDtypeStruct((3, atoms), F32),
        ),
        in_specs=[vmem] * 6 + [smem] * 2 + [hbm] * 5 + [vmem] * 2,
        out_specs=(hbm, vmem),
        scratch_shapes=scratch,
        compiler_params=pltpu.CompilerParams(collective_id=0, has_side_effects=True),
    )(
        jnp.transpose(embeddings, (1, 0, 2)),
        row(neighbours),
        row(valid),
        row(azimuth),
        row(polar),
        row(distance),
        send_low,
        send_high,
        *weights,
        radial_weight,
        readout.reshape(1, channels),
    )
    updated, forces = pl.pallas_call(
        hand_over,
        out_shape=(
            jax.ShapeDtypeStruct(updated.shape, BF16),
            jax.ShapeDtypeStruct(forces.shape, F32),
        ),
        in_specs=[vmem, vmem],
        out_specs=(vmem, vmem),
    )(updated, forces)
    return (jnp.transpose(updated, (1, 0, 2)), forces)


def solution(mesh):
    both = ("slab", "yz")
    in_specs = (P(both, None, None),) + (P(both),) * 7 + (P(),) * 7
    out_specs = (P(both, None, None), P(None, both))
    return jax.shard_map(
        functools.partial(body, mesh.shape["slab"], mesh.shape["yz"]),
        mesh=mesh,
        in_specs=in_specs,
        out_specs=out_specs,
        check_vma=False,
    )
```

```python
import functools
import math

import jax
import jax.numpy as jnp
from jax import lax
from jax.experimental import pallas as pl
from jax.experimental.pallas import tpu as pltpu
from jax.sharding import PartitionSpec as P

LAYERS = 2
MESH = pl.DeviceIdType.MESH
HIGHEST = lax.Precision.HIGHEST
F32 = jnp.float32
BF16 = jnp.bfloat16


def slot_index(degree, order):
    return degree * degree + degree + order


def slot_groups(degrees):
    groups = [[slot_index(degree, 0) for degree in range(degrees)]]
    for order in (1, 2):
        groups.append(
            [slot_index(degree, order) for degree in range(order, degrees)]
            + [slot_index(degree, -order) for degree in range(order, degrees)]
        )
    return groups


def nt_dot(left, right, precision=None):
    return lax.dot_general(
        left, right, (((1,), (1,)), ((), ())), precision=precision, preferred_element_type=F32
    )


def thirds(values):
    head = values.astype(BF16).astype(F32)
    mid = (values - head).astype(BF16).astype(F32)
    return head, mid, values - head - mid


def thirds_dot(values, exact):
    rows = jnp.concatenate(thirds(values), axis=0).astype(BF16)
    total = nt_dot(rows, exact)
    count = values.shape[0]
    return total[:count] + (total[count : 2 * count] + total[2 * count :])


def kernel(
    n_slab,
    n_yz,
    atoms,
    coeffs,
    channels,
    ghosts,
    neighb,
    groups,
    emb,
    nbr,
    val,
    azi,
    pol,
    dist,
    send_low,
    send_high,
    w_hbm0,
    w_hbm1,
    w_hbm2,
    w_hbm3,
    w_hbm4,
    radial_weight,
    readout,
    out_e,
    out_f,
    wv0,
    wv1,
    wv2,
    wv3,
    wv4,
    natural,
    radp,
    picks,
    scatter,
    direction,
    chooser,
    f_send,
    f_recv,
    *rest,
):
    n_groups = len(groups)
    own_bufs = [rest[layer * n_groups : (layer + 1) * n_groups] for layer in range(LAYERS)]
    rest = rest[LAYERS * n_groups :]
    ghost_bufs = [rest[layer * n_groups : (layer + 1) * n_groups] for layer in range(LAYERS)]
    rest = rest[LAYERS * n_groups :]
    lend_bufs = [rest[layer * n_groups : (layer + 1) * n_groups] for layer in range(LAYERS)]
    rest = rest[LAYERS * n_groups :]
    weight_sem, send_sem, recv_sem = rest

    edges = atoms * neighb
    own_rows = n_yz * atoms
    ghost_rows = n_yz * ghosts
    table_rows = own_rows + 2 * ghost_rows
    half = n_yz // 2

    slab = lax.axis_index("slab")
    q = lax.axis_index("yz")
    above = lax.rem(slab + 1, n_slab)
    below = lax.rem(slab + n_slab - 1, n_slab)
    core = lax.rem(q, 2)
    row = q // 2
    partner = q + 1 - 2 * core

    def to_peer(j):
        return lax.rem(row + j, half) * 2 + core

    def from_peer(j):
        return lax.rem(row + half - j, half) * 2 + core

    def partner_of(index):
        return index + 1 - 2 * lax.rem(index, 2)

    weight_pairs = ((w_hbm0, wv0), (w_hbm1, wv1), (w_hbm2, wv2), (w_hbm3, wv3), (w_hbm4, wv4))
    weight_copies = [
        [
            pltpu.make_async_copy(
                source.at[layer], target.at[layer], weight_sem.at[layer * 5 + number]
            )
            for number, (source, target) in enumerate(weight_pairs)
        ]
        for layer in range(LAYERS)
    ]
    for layer in range(LAYERS):
        for copy in weight_copies[layer]:
            copy.start()

    barrier = pltpu.get_barrier_semaphore()
    peers = [(slab, lax.rem(q + j, n_yz)) for j in range(1, n_yz)]
    peers += [(above, lax.rem(q + j, n_yz)) for j in range(n_yz)]
    peers += [(below, lax.rem(q + j, n_yz)) for j in range(n_yz)]
    for peer in peers:
        pl.semaphore_signal(barrier, inc=1, device_id=peer, device_id_type=MESH)

    lend_row = lax.broadcasted_iota(jnp.int32, (2 * ghosts, atoms), 0)
    lend_col = lax.broadcasted_iota(jnp.int32, (2 * ghosts, atoms), 1)
    wanted = jnp.zeros((2 * ghosts, atoms), jnp.int32)
    for g in range(ghosts):
        wanted = jnp.where(lend_row == g, send_high[g], wanted)
        wanted = jnp.where(lend_row == ghosts + g, send_low[g], wanted)
    lend = (wanted == lend_col).astype(F32).astype(BF16)

    def lend_rows(layer, number):
        rows = jnp.dot(lend, own_bufs[layer][number][q], preferred_element_type=F32)
        lend_bufs[layer][number][0] = rows[:ghosts].astype(BF16)
        lend_bufs[layer][number][1] = rows[ghosts:].astype(BF16)

    for number, group in enumerate(groups):
        for place, slot in enumerate(group):
            own_bufs[0][number][q, :, place * channels : (place + 1) * channels] = emb[slot]
        lend_rows(0, number)

    pl.semaphore_wait(barrier, len(peers))

    sends = []
    count = [0]

    def send(source, target, device):
        k = count[0]
        count[0] += 1
        copy = pltpu.make_async_remote_copy(
            src_ref=source,
            dst_ref=target,
            send_sem=send_sem.at[k],
            recv_sem=recv_sem.at[k],
            device_id=device,
            device_id_type=MESH,
        )
        copy.start()
        sends.append(copy)
        return k

    def arrive(k, target):
        pltpu.make_async_remote_copy(
            src_ref=target,
            dst_ref=target,
            send_sem=send_sem.at[k],
            recv_sem=recv_sem.at[k],
            device_id=(slab, partner),
            device_id_type=MESH,
        ).wait_recv()

    marks = {}

    def stage_a(layer, number):
        own, ghost, lent = (
            own_bufs[layer][number],
            ghost_bufs[layer][number],
            lend_bufs[layer][number],
        )
        marks["up", layer, number] = send(lent.at[0], ghost.at[q, 0], (above, q))
        marks["down", layer, number] = send(lent.at[1], ghost.at[q, 1], (below, q))
        for j in range(1, half):
            marks["own", layer, number, j] = send(own.at[q], own.at[q], (slab, to_peer(j)))
        marks["own", layer, number, 0] = send(own.at[q], own.at[q], (slab, partner))

    def stage_b(layer, number):
        own = own_bufs[layer][number]
        for j in range(1, half):
            source = from_peer(j)
            arrive(marks["own", layer, number, j], own.at[source])
            marks["own2", layer, number, j] = send(
                own.at[source], own.at[source], (slab, partner)
            )

    def stage_c(layer, number):
        ghost = ghost_bufs[layer][number]
        arrive(marks["up", layer, number], ghost.at[q, 0])
        arrive(marks["down", layer, number], ghost.at[q, 1])
        for j in range(1, half):
            marks["ghost", layer, number, j] = send(
                ghost.at[q], ghost.at[q], (slab, to_peer(j))
            )
        marks["ghost", layer, number, 0] = send(ghost.at[q], ghost.at[q], (slab, partner))

    def stage_d(layer, number):
        ghost = ghost_bufs[layer][number]
        for j in range(1, half):
            source = from_peer(j)
            arrive(marks["ghost", layer, number, j], ghost.at[source])
            marks["ghost2", layer, number, j] = send(
                ghost.at[source], ghost.at[source], (slab, partner)
            )

    def stage_w(layer, number):
        own, ghost = own_bufs[layer][number], ghost_bufs[layer][number]
        arrive(marks["own", layer, number, 0], own.at[partner])
        arrive(marks["ghost", layer, number, 0], ghost.at[partner])
        for j in range(1, half):
            source = partner_of(from_peer(j))
            arrive(marks["own2", layer, number, j], own.at[source])
            arrive(marks["ghost2", layer, number, j], ghost.at[source])

    def table_of(layer, number):
        own, ghost = own_bufs[layer][number], ghost_bufs[layer][number]
        blocks = [own[index] for index in range(n_yz)]
        lent = [ghost[index, 0].astype(F32) for index in range(n_yz)]
        lent += [ghost[index, 1].astype(F32) for index in range(n_yz)]
        return jnp.concatenate(blocks + [jnp.concatenate(lent, axis=0).astype(BF16)], axis=0)

    def mixed(layer, number):
        table = table_of(layer, number)
        if number == 0:
            return jnp.dot(table, wv0[layer], preferred_element_type=F32).astype(BF16)
        real, imag = ((wv1, wv2), (wv3, wv4))[number - 1]
        width = table.shape[1] // 2
        stacked = jnp.concatenate([table[:, :width], table[:, width:]], axis=0)
        by_real = jnp.dot(stacked, real[layer], preferred_element_type=F32)
        by_imag = jnp.dot(stacked, imag[layer], preferred_element_type=F32)
        plus = by_real[:table_rows] - by_imag[table_rows:]
        minus = by_imag[:table_rows] + by_real[table_rows:]
        return jnp.concatenate([plus.astype(BF16), minus.astype(BF16)], axis=1)

    def compute(layer, number):
        group = groups[number]
        mix = mixed(layer, number)
        last = layer == LAYERS - 1
        for first in range(0, len(group), 2):
            places = list(range(first, min(first + 2, len(group))))
            columns = slice(places[0] * channels, (places[-1] + 1) * channels)
            gathered = jnp.dot(picks[...], mix[:, columns], preferred_element_type=F32)
            for position, place in enumerate(places):
                part = gathered[:, position * channels : (position + 1) * channels] * radp[layer]
                if last and number == 0 and place == 0:
                    for slot in range(neighb):
                        natural[pl.ds(slot, atoms, stride=neighb), :] = part[
                            slot * atoms : (slot + 1) * atoms
                        ]
                total = part.reshape(neighb, atoms, channels).sum(axis=0)
                lanes = slice(place * channels, (place + 1) * channels)
                fresh = (
                    own_bufs[layer][number][q, :, lanes].astype(F32) + 0.18 * total
                ).astype(BF16)
                if last:
                    out_e[group[place]] = fresh
                else:
                    own_bufs[layer + 1][number][q, :, lanes] = fresh

    def permuted(store):
        for slot in range(neighb):
            store(
                slice(slot * atoms, (slot + 1) * atoms),
                natural[pl.ds(slot, atoms, stride=neighb), :],
            )

    for number in range(n_groups):
        stage_a(0, number)

    bases = radial_weight.shape[1]
    centers = 1.0 + 0.5 * lax.broadcasted_iota(jnp.int32, (bases, edges), 0).astype(F32)
    basis = jnp.exp(-jnp.square((dist[...] - centers) / 0.5)).T
    row_ids = lax.broadcasted_iota(jnp.int32, (table_rows, edges), 0)
    hot = jnp.where((row_ids == nbr[...]) & (val[...] != 0), 1.0, 0.0).astype(F32)
    scatter[:table_rows, :] = hot.astype(BF16)
    natural[...] = hot.T

    def keep_picks(rows, values):
        picks[rows, :] = values.astype(BF16)

    permuted(keep_picks)
    for layer in range(LAYERS):
        pre = jnp.dot(basis, radial_weight[layer], precision=HIGHEST, preferred_element_type=F32)
        natural[...] = pre / (1.0 + jnp.exp(-pre))

        def keep_radial(rows, values, layer=layer):
            radp[layer, rows, :] = values

        permuted(keep_radial)

    for number in range(n_groups):
        stage_b(0, number)

    atom_ids = lax.broadcasted_iota(jnp.int32, (atoms, edges), 0)
    edge_ids = lax.broadcasted_iota(jnp.int32, (atoms, edges), 1)
    mine = (edge_ids >= atom_ids * neighb) & (edge_ids < (atom_ids + 1) * neighb)
    scatter[table_rows:, :] = jnp.where(mine, 1.0, 0.0).astype(F32).astype(BF16)
    sin_polar = jnp.sin(pol[...])
    part_ids = lax.broadcasted_iota(jnp.int32, (8, edges), 0)
    direction[...] = jnp.where(
        part_ids == 0,
        sin_polar * jnp.cos(azi[...]),
        jnp.where(
            part_ids == 1,
            sin_polar * jnp.sin(azi[...]),
            jnp.where(part_ids == 2, jnp.cos(pol[...]), 0.0),
        ),
    )

    table_ids = lax.broadcasted_iota(jnp.int32, (atoms, table_rows), 1)
    owner_ids = lax.broadcasted_iota(jnp.int32, (atoms, table_rows), 0)
    pick = table_ids == q * atoms + owner_ids
    for g in range(ghosts):
        pick |= (table_ids == own_rows + q * ghosts + g) & (owner_ids == send_high[g])
        pick |= (table_ids == own_rows + ghost_rows + q * ghosts + g) & (
            owner_ids == send_low[g]
        )
    chooser[...] = jnp.where(pick, 1.0, 0.0).astype(F32).astype(BF16)

    used = {slot for group in groups for slot in group}
    for slot in range(coeffs):
        if slot not in used:
            out_e[slot] = emb[slot]

    for number in range(n_groups):
        stage_c(0, number)
    for number in range(n_groups):
        stage_d(0, number)
    for copy in weight_copies[0]:
        copy.wait()
    for number in range(n_groups):
        stage_w(0, number)
        compute(0, number)
        lend_rows(1, number)
        stage_a(1, number)
    for copy in weight_copies[1]:
        copy.wait()
    for number in range(n_groups):
        stage_b(1, number)
        stage_c(1, number)

    force_marks = {}
    for number in range(n_groups):
        stage_d(1, number)
    for number in range(n_groups):
        stage_w(1, number)
        compute(1, number)
        if number == 0:
            tall = jnp.broadcast_to(readout[...], (8, channels))
            tall_head, tall_mid, tall_tail = thirds(tall)
            tall_rows = jnp.concatenate([tall_head, tall_mid, tall_tail], axis=0).astype(BF16)
            scalar_head, scalar_mid, scalar_tail = thirds(natural[...])
            total = nt_dot(tall_rows, scalar_head.astype(BF16))
            total += nt_dot(tall_rows, scalar_mid.astype(BF16))
            total += nt_dot(tall_rows, scalar_tail.astype(BF16))
            strength = 0.125 * (total[:8] + (total[8:16] + total[16:24]))
            parts = thirds_dot(direction[...] * strength, scatter[...])
            own_force = parts[:, table_rows:]
            f_send[...] = -parts[:, :table_rows]
            order = list(range(n_yz - 1, len(peers))) + list(range(n_yz - 1))
            for index in order:
                force_marks[index] = send(f_send, f_recv.at[index], peers[index])

    for index, k in force_marks.items():
        arrive(k, f_recv.at[index])
    own_sum = f_send[...]
    for index in range(n_yz - 1):
        own_sum = own_sum + f_recv[index]
    below_sum = f_recv[n_yz - 1]
    above_sum = f_recv[2 * n_yz - 1]
    for index in range(1, n_yz):
        below_sum = below_sum + f_recv[n_yz - 1 + index]
        above_sum = above_sum + f_recv[2 * n_yz - 1 + index]
    lane = lax.broadcasted_iota(jnp.int32, (8, table_rows), 1)
    returned = jnp.where(
        lane < own_rows,
        own_sum,
        jnp.where(lane < own_rows + ghost_rows, above_sum, below_sum),
    )
    out_f[...] = (own_force + thirds_dot(returned, chooser[...]))[:3]

    for copy in sends:
        copy.wait_send()


def hand_over(rows, forces, rows_out, forces_out):
    rows_out[...] = rows[...]
    forces_out[...] = forces[...]


def body(
    n_slab,
    n_yz,
    embeddings,
    neighbours,
    valid,
    azimuth,
    polar,
    distance,
    send_low,
    send_high,
    w_zero,
    w_one_re,
    w_one_im,
    w_two_re,
    w_two_im,
    radial_weight,
    readout,
):
    atoms, coeffs, channels = embeddings.shape
    degrees = math.isqrt(coeffs)
    edges = neighbours.shape[0]
    neighb = edges // atoms
    ghosts = send_low.shape[0]
    groups = slot_groups(degrees)
    table_rows = n_yz * (atoms + 2 * ghosts)
    widths = [len(group) * channels for group in groups]
    weights = (w_zero, w_one_re, w_one_im, w_two_re, w_two_im)
    n_peers = 3 * n_yz - 1
    half = n_yz // 2
    copies = LAYERS * len(groups) * (2 + 2 * half + 2 * (half - 1)) + n_peers
    vmem = pl.BlockSpec(memory_space=pltpu.VMEM)
    smem = pl.BlockSpec(memory_space=pltpu.SMEM)
    hbm = pl.BlockSpec(memory_space=pl.ANY)
    row = lambda array: array.reshape(1, edges)
    scratch = [pltpu.VMEM(weight.shape, BF16) for weight in weights]
    scratch += [
        pltpu.VMEM((edges, channels), F32),
        pltpu.VMEM((LAYERS, edges, channels), F32),
        pltpu.VMEM((edges, table_rows), BF16),
        pltpu.VMEM((table_rows + atoms, edges), BF16),
        pltpu.VMEM((8, edges), F32),
        pltpu.VMEM((atoms, table_rows), BF16),
        pltpu.VMEM((8, table_rows), F32),
        pltpu.VMEM((n_peers, 8, table_rows), F32),
    ]
    for _ in range(LAYERS):
        scratch += [pltpu.VMEM((n_yz, atoms, width), BF16) for width in widths]
    for _ in range(LAYERS):
        scratch += [pltpu.VMEM((n_yz, 2, ghosts, width), BF16) for width in widths]
    for _ in range(LAYERS):
        scratch += [pltpu.VMEM((2, ghosts, width), BF16) for width in widths]
    scratch += [
        pltpu.SemaphoreType.DMA((5 * LAYERS,)),
        pltpu.SemaphoreType.DMA((copies,)),
        pltpu.SemaphoreType.DMA((copies,)),
    ]
    updated, forces = pl.pallas_call(
        functools.partial(
            kernel, n_slab, n_yz, atoms, coeffs, channels, ghosts, neighb, groups
        ),
        out_shape=(
            pltpu.VMEM((coeffs, atoms, channels), BF16),
            pltpu.VMEM((3, atoms), F32),
        ),
        in_specs=[vmem] * 6 + [smem] * 2 + [hbm] * 5 + [vmem] * 2,
        out_specs=(vmem, vmem),
        scratch_shapes=scratch,
        compiler_params=pltpu.CompilerParams(collective_id=0, has_side_effects=True),
    )(
        jnp.transpose(embeddings, (1, 0, 2)),
        row(neighbours),
        row(valid),
        row(azimuth),
        row(polar),
        row(distance),
        send_low,
        send_high,
        *weights,
        radial_weight,
        readout.reshape(1, channels),
    )
    updated, forces = pl.pallas_call(
        hand_over,
        out_shape=(
            jax.ShapeDtypeStruct(updated.shape, BF16),
            jax.ShapeDtypeStruct(forces.shape, F32),
        ),
        in_specs=[vmem, vmem],
        out_specs=(vmem, vmem),
    )(
        pltpu.with_memory_space_constraint(updated, pltpu.VMEM),
        pltpu.with_memory_space_constraint(forces, pltpu.VMEM),
    )
    return (jnp.transpose(updated, (1, 0, 2)), forces)


def solution(mesh):
    both = ("slab", "yz")
    in_specs = (P(both, None, None),) + (P(both),) * 7 + (P(),) * 7
    out_specs = (P(both, None, None), P(None, both))
    return jax.shard_map(
        functools.partial(body, mesh.shape["slab"], mesh.shape["yz"]),
        mesh=mesh,
        in_specs=in_specs,
        out_specs=out_specs,
        check_vma=False,
    )
```
